32 devices in a mesh: dp: 16 (over z, y, x), mp: 2 (over core).
Axes of the slice: x: 2, y: 2, z: 4, core: 2. Of those that a mesh axis runs over, the one named last changes fastest.
Arguments:
- inputs: bfloat16 [16, 2, 256, 2048], P('dp'), may hold values from -6 to 6
- grad_out: bfloat16 [16, 2, 256, 256], P('dp', None, None, 'mp'), parts along dimension 3, may hold values from -0.5 to 0.5
- momentum: float32 [16, 2048, 256], P('dp', None, 'mp'), parts along dimension 2, may hold values from -6 to 6
- select: int32 [16, 2, 16, 16], P(None, None, None, 'mp'), parts along dimension 3, may hold values from -1 to 127, as said below
Outputs:
- update: bfloat16 [2048, 256], P(None, 'mp'), parts along dimension 1
- new_momentum: float32 [16, 2048, 256], P('dp', None, 'mp'), parts along dimension 2
The draws below stay inside these ranges and needn't reach their ends.
There are 2 independent parts, one for each index of `mp`. The reference program is written for one: setup_inputs(seed, part) draws one part's arguments, and reference() takes and returns one part's arrays. A program takes and returns all parts, laid end to end along the dimension named above; an argument that names none is the same for every part. Nothing has to cross between parts.
Inputs may be any that keep to these rules, and one draw needn't show every extreme that they name: `select`: in each [r, s, o] list the entries that are not -1 are distinct and come first. In every step some owner gets exactly 8 rows from every replica.
All inputs are finite; a program needn't handle non-finite values.
Results may differ from the reference program's by a relative error of at most 0.001.
Values sent between devices are 32-bit elements; how exact they have to be, the bound alone decides.
No kernel may reach another device: no remote copies, remote signals or barrier semaphores. Data moves between devices by JAX's collectives and lax.ppermute only.
A program may use at most 64 MiB of HBM per device.

```python
import jax
import jax.numpy as jnp
from jax import lax

ROWS = 2048
COLS = 128
GROUP = 64
TOK = 256
STEPS = 2
CAP = 8
REPLICAS = 16
N_DP = 16


def draw_select(key, part):
    key_tier, key_hot, key_count, key_order = jax.random.split(jax.random.fold_in(key, 7), 4)
    per_owner = ROWS // N_DP
    tier = jax.random.randint(key_tier, (1, STEPS, REPLICAS, 1), 0, 3)
    hottest = jax.random.randint(key_hot, (1, STEPS, 1, 1), 0, REPLICAS)
    drawn = jax.random.randint(key_count, (REPLICAS, STEPS, REPLICAS, 1), 0, CAP + 1)
    counts = jnp.minimum(CAP, drawn * tier // 2)
    owner_ids = lax.broadcasted_iota(jnp.int32, (1, STEPS, REPLICAS, 1), 2)
    counts = jnp.where(owner_ids == hottest, CAP, counts)
    scores = jax.random.randint(key_order, (REPLICAS, STEPS, REPLICAS, per_owner), 0, 1 << 20) * per_owner
    scores = scores + lax.broadcasted_iota(jnp.int32, (REPLICAS, STEPS, REPLICAS, per_owner), 3)
    ordering = jnp.argsort(scores, axis=3)[..., :CAP].astype(jnp.int32)
    slots = lax.broadcasted_iota(jnp.int32, (REPLICAS, STEPS, REPLICAS, CAP), 3)
    return jnp.where(slots < counts, ordering, -1).astype(jnp.int32)


def block_levels(own_key, shape, pieces, low, high):
    def one(axis_at, blocks):
        heights = jax.random.uniform(jax.random.fold_in(jax.random.fold_in(own_key, 6), axis_at), (blocks,), jnp.float32, low / len(pieces), high / len(pieces))
        return jnp.repeat(jnp.exp(heights), shape[axis_at] // blocks).reshape((-1,) + (1,) * (len(shape) - axis_at - 1))

    loudness = one(*pieces[0])
    for cut in pieces[1:]:
        loudness = loudness * one(*cut)
    return loudness


def scatter_about(own_key, dims, width, limit, pieces=(), held_as=jnp.bfloat16):
    values = jax.random.normal(own_key, dims, jnp.float32) * width
    if len(pieces) > 0:
        values = block_levels(own_key, dims, pieces, -0.22, 0.18) * values
    return jnp.clip(values, min=-limit, max=limit).astype(held_as)


def setup_inputs(seed: int = 0, part: int = 0) -> dict:
    arg_keys = jax.random.split(jax.random.key(seed), 5)
    part_keys = jax.random.split(jax.random.fold_in(arg_keys[4], part), 5)
    return {
        "inputs": scatter_about(arg_keys[0], (REPLICAS, STEPS, TOK, ROWS), 1.0, 6.0, ((0, 16),)),
        "grad_out": scatter_about(part_keys[1], (REPLICAS, STEPS, TOK, COLS), 0.0625, 0.5, ((0, 16),)),
        "momentum": scatter_about(part_keys[2], (REPLICAS, ROWS, COLS), 1.0, 6.0, ((0, 16),), jnp.float32),
        "select": draw_select(jax.random.fold_in(jax.random.fold_in(arg_keys[4], part), 71), part),
    }


def dct_matrix(order):
    freq = lax.broadcasted_iota(jnp.int32, (order, order), 0).astype(jnp.float32)
    place = lax.broadcasted_iota(jnp.int32, (order, order), 1).astype(jnp.float32)
    factor = jnp.where(freq == 0.0, jnp.sqrt(1.0 / order), jnp.sqrt(2.0 / order)).astype(jnp.float32)
    return factor * jnp.cos(jnp.pi * (2.0 * place + 1.0) * freq / (2.0 * order))

def forward_blocks(field, dct_table, col_table):
    replicas = field.shape[0]
    shaped = field.reshape(replicas, ROWS // GROUP, GROUP, COLS)
    rowwise = jnp.einsum('ui,raic->rauc', dct_table, shaped, precision=lax.Precision.HIGHEST)
    rowwise = rowwise.reshape(replicas, ROWS, COLS)
    return jnp.einsum('rkc,vc->rkv', rowwise, col_table, precision=lax.Precision.HIGHEST)

def inverse_blocks(coeffs, dct_table, col_table):
    replicas = coeffs.shape[0]
    colwise = jnp.einsum('rkv,vc->rkc', coeffs, col_table, precision=lax.Precision.HIGHEST)
    shaped = colwise.reshape(replicas, ROWS // GROUP, GROUP, COLS)
    back = jnp.einsum('ui,rauc->raic', dct_table, shaped, precision=lax.Precision.HIGHEST)
    return back.reshape(replicas, ROWS, COLS)

def reference(inputs, grad_out, momentum, select):
    dct_table = dct_matrix(GROUP)
    col_table = jnp.kron(jnp.eye(COLS // GROUP, dtype=jnp.float32), dct_table)
    replicas = momentum.shape[0]
    per_owner = ROWS // N_DP
    moment_state = momentum
    update_sum = jnp.zeros((ROWS, COLS), jnp.float32)
    owner_base = (lax.broadcasted_iota(jnp.int32, (replicas, select.shape[2], CAP), 1) * per_owner).astype(jnp.int32)
    replica_rows = lax.broadcasted_iota(jnp.int32, (replicas, select.shape[2] * CAP), 0)
    for iteration in range(STEPS):
        gradient = jnp.einsum('rtk,rtc->rkc', inputs[:, iteration].astype(jnp.float32), grad_out[:, iteration].astype(jnp.float32), precision=lax.Precision.HIGHEST)
        moment_state = 0.999 * moment_state + gradient
        coefficients = forward_blocks(moment_state, dct_table, col_table)
        listed = select[:, iteration]
        global_rows = jnp.where(listed >= 0, listed + owner_base, ROWS).astype(jnp.int32)
        chosen = jnp.zeros((replicas, ROWS + 1), jnp.float32)
        chosen = chosen.at[replica_rows, global_rows.reshape(replicas, -1)].set(1.0)[:, :ROWS]
        sent = coefficients * chosen[:, :, None]
        summed = lax.optimization_barrier(jnp.sum(sent, axis=0))
        update_sum = update_sum + inverse_blocks(summed[None], dct_table, col_table)[0]
        moment_state = moment_state - inverse_blocks(sent, dct_table, col_table)
    return (update_sum.astype(jnp.bfloat16), moment_state)
```

```python
import functools

import jax
import jax.numpy as jnp
import numpy as np
from jax import lax
from jax.experimental import pallas as pl
from jax.experimental.pallas import tpu as pltpu
from jax.sharding import PartitionSpec as P

GROUP = 64
TILE = 2 * GROUP
CHUNKS = 4
F32 = jnp.float32
BF16 = jnp.bfloat16
VMEM = pl.BlockSpec(memory_space=pltpu.VMEM)
SMEM = pl.BlockSpec(memory_space=pltpu.SMEM)
ANY = pl.BlockSpec(memory_space=pl.ANY)


def block_dct(size):
    freq = np.arange(GROUP)[:, None]
    place = np.arange(GROUP)[None, :]
    factor = np.where(freq == 0, np.sqrt(1.0 / GROUP), np.sqrt(2.0 / GROUP))
    table = factor * np.cos(np.pi * (2.0 * place + 1.0) * freq / (2.0 * GROUP))
    return np.kron(np.eye(size // GROUP), table)


def halves(matrix):
    high = matrix.astype(jnp.bfloat16)
    low = (matrix - high.astype(np.float64)).astype(jnp.bfloat16)
    return high, low


def left_table(matrix):
    high, low = halves(matrix)
    return np.block([[high, high], [low, low]])


def right_table(matrix):
    high, low = halves(matrix)
    return np.block([[high, low], [high, low]])


def split(value, axis):
    high = value.astype(BF16)
    low = (value - high.astype(F32)).astype(BF16)
    return jnp.concatenate([high, low], axis=axis)


def mm(a, b):
    return jnp.dot(a, b, preferred_element_type=F32)


def mm_t(a, b):
    return lax.dot_general(a, b, (((0,), (0,)), ((), ())), preferred_element_type=F32)


def right(value, table):
    both = mm(split(value, 1), table)
    half = both.shape[1] // 2
    return both[:, :half] + both[:, half:]


def left(table, value):
    both = mm(table, split(value, 0))
    half = both.shape[0] // 2
    return both[:half] + both[half:]


def forward_kernel(index, x_hbm, g, m_hbm, row_t, col_t, picks, rest, x, m, c1, f2, sems):
    rows, cols = m.shape
    slots = index.shape[0] // 2
    width = rows // CHUNKS
    copies = []
    for c in range(CHUNKS):
        span = pl.ds(c * width, width)
        a = pltpu.make_async_copy(x_hbm.at[:, :, span], x.at[:, :, span], sems.at[c, 0])
        b = pltpu.make_async_copy(m_hbm.at[span], m.at[span], sems.at[c, 1])
        a.start()
        b.start()
        copies.append((a, b))
    c1[pl.ds(rows, 8), :] = jnp.zeros((8, cols), F32)
    rest[pl.ds(rows, 8), :] = jnp.zeros((8, cols), F32)
    table = col_t[...]
    row_table = row_t[...]
    second = mm(g[1], table[:cols])
    second = split(second[:, :cols] + second[:, cols:], 1)
    first = g[0]
    for c in range(CHUNKS):
        copies[c][0].wait()
        copies[c][1].wait()
        for r in range(c * width, (c + 1) * width, TILE):
            m1 = 0.999 * m[r : r + TILE] + mm_t(x[0, :, r : r + TILE], first)
            y1 = right(m1, table)
            y2 = mm_t(x[1, :, r : r + TILE], second)
            y2 = y2[:, :cols] + y2[:, cols:]
            z = left(row_table, jnp.concatenate([y1, y2], axis=1))
            c1[r : r + TILE] = z[:, :cols]
            f2[r : r + TILE] = z[:, cols:]
    per = picks.shape[1] // 2
    for k in range(slots):
        picks[k // per, pl.ds(k % per, 1), :] = c1[pl.ds(index[k], 1), :]
    zero = jnp.zeros((1, cols), F32)
    for k in range(slots):
        c1[pl.ds(index[k], 1), :] = zero
    rest[:rows] = 0.999 * c1[:rows] + f2[...]
    for k in range(slots):
        picks[k // per, pl.ds(per + k % per, 1), :] = rest[pl.ds(index[slots + k], 1), :]
    for k in range(slots):
        rest[pl.ds(index[slots + k], 1), :] = zero


def forward(index, x, g, m, slots):
    rows, cols = m.shape
    steps, tokens, _ = x.shape
    owners = index.shape[0] // (steps * slots)
    row_t = jnp.asarray(left_table(block_dct(TILE)))
    col_t = jnp.asarray(right_table(block_dct(cols).T))
    return pl.pallas_call(
        forward_kernel,
        out_shape=(
            jax.ShapeDtypeStruct((owners, steps * slots, cols), F32),
            jax.ShapeDtypeStruct((rows + 8, cols), F32),
        ),
        in_specs=[SMEM, ANY, VMEM, ANY, VMEM, VMEM],
        out_specs=(VMEM, VMEM),
        scratch_shapes=[
            pltpu.VMEM(x.shape, x.dtype),
            pltpu.VMEM((rows, cols), F32),
            pltpu.VMEM((rows + 8, cols), F32),
            pltpu.VMEM((rows, cols), F32),
            pltpu.SemaphoreType.DMA((CHUNKS, 2)),
        ],
        name="forward",
    )(index, x, g, m, row_t, col_t)


def inverse_tile(value, row_table, col_table):
    return left(row_table, right(value, col_table))


def inverse_kernel(coeffs, row_t, col_t, out):
    row_table, table = row_t[...], col_t[...]
    for r in range(0, out.shape[0], TILE):
        out[r : r + TILE] = inverse_tile(coeffs[r : r + TILE], row_table, table)


def inverse_tables(cols):
    return (
        jnp.asarray(left_table(block_dct(TILE).T)),
        jnp.asarray(right_table(block_dct(cols))),
    )


def inverse(coeffs, rows):
    cols = coeffs.shape[1]
    return pl.pallas_call(
        inverse_kernel,
        out_shape=jax.ShapeDtypeStruct((rows, cols), F32),
        in_specs=[VMEM] * 3,
        out_specs=VMEM,
        name="inverse",
    )(coeffs, *inverse_tables(cols))


def owned_kernel(whole, listed, arrived, row_t, col_t, out):
    rows, cols = out.shape
    slots = listed.shape[1]
    ids = lax.broadcasted_iota(jnp.int32, (rows, slots), 0)
    onehot = jnp.where(ids == listed[...], 1.0, 0.0).astype(BF16)
    both = mm(onehot, split(arrived[...].reshape(slots, cols), 1))
    summed = both[:, :cols] + both[:, cols:]
    if whole:
        for r in range(0, rows, TILE):
            out[r : r + TILE] = inverse_tile(summed[r : r + TILE], row_t[...], col_t[...])
    else:
        out[...] = summed


def owned_rows(listed, arrived, per_owner):
    cols = arrived.shape[-1]
    return pl.pallas_call(
        functools.partial(owned_kernel, per_owner % TILE == 0),
        out_shape=jax.ShapeDtypeStruct((per_owner, cols), F32),
        in_specs=[VMEM] * 4,
        out_specs=VMEM,
        name="owned",
    )(listed, arrived, *inverse_tables(cols))


def finish_kernel(whole, inner, me, row_t, col_t, *refs):
    blocks, out = refs[:-1], refs[-1]
    outer = blocks[0].shape[0]
    high, low = me[0] // inner, me[0] % inner
    for j, block in enumerate(blocks):
        for k in range(outer):
            place = (high ^ k) * inner + (low ^ j)
            out[place] = block[k].astype(out.dtype)


def finish(blocks, me, inner):
    outer, per_owner, cols = blocks[0].shape
    whole = per_owner % TILE == 0
    dtype = BF16 if whole else F32
    out = pl.pallas_call(
        functools.partial(finish_kernel, whole, inner),
        out_shape=jax.ShapeDtypeStruct((outer * inner, per_owner, cols), dtype),
        in_specs=[SMEM] + [VMEM] * (2 + len(blocks)),
        out_specs=VMEM,
        name="finish",
    )(me, *inverse_tables(cols), *blocks)
    out = out.reshape(outer * inner * per_owner, cols)
    if not whole:
        out = inverse(out, out.shape[0]).astype(BF16)
    return out


def per_device(inputs, grad_out, momentum, select):
    replica = lax.axis_index("dp")
    owners = lax.axis_size("dp")
    steps = inputs.shape[1]
    rows, cols = momentum.shape[1:]
    per_owner = rows // owners
    slots = select.shape[3]
    inner = 1
    while inner * inner < owners:
        inner *= 2
    outer = owners // inner

    own = lax.dynamic_index_in_dim(select, replica, 0, keepdims=False)
    base = lax.broadcasted_iota(jnp.int32, own.shape, 1) * per_owner
    index = jnp.where(own >= 0, own + base, rows).reshape(-1)
    picks, rest = forward(index, inputs[0], grad_out[0], momentum[0], slots)
    arrived = lax.all_to_all(picks, "dp", split_axis=0, concat_axis=0, tiled=True)

    new_momentum = inverse(rest, rows)
    listed = lax.dynamic_index_in_dim(select, replica, 2, keepdims=False).reshape(1, -1)
    mine = owned_rows(listed, arrived, per_owner)

    def from_peer(value, shift):
        return lax.ppermute(value, "dp", [(d, d ^ shift) for d in range(owners)])

    column = jnp.stack([mine] + [from_peer(mine, k * inner) for k in range(1, outer)])
    blocks = [column] + [from_peer(column, j) for j in range(1, inner)]
    update = finish(blocks, replica.reshape(1).astype(jnp.int32), inner)
    return (update, new_momentum[None])


def solution(mesh):
    return jax.shard_map(
        per_device,
        mesh=mesh,
        in_specs=(
            P("dp", None, None, None),
            P("dp", None, None, "mp"),
            P("dp", None, "mp"),
            P(None, None, None, "mp"),
        ),
        out_specs=(P(None, "mp"), P("dp", None, "mp")),
        check_vma=False,
    )
```

```python
import functools

import jax
import jax.numpy as jnp
import numpy as np
from jax import lax
from jax.experimental import pallas as pl
from jax.experimental.pallas import tpu as pltpu
from jax.sharding import PartitionSpec as P

GROUP = 64
CHUNKS = 4
F32 = jnp.float32
BF16 = jnp.bfloat16
IN_VMEM = pl.BlockSpec(memory_space=pltpu.VMEM)
IN_HBM = pl.BlockSpec(memory_space=pltpu.HBM)
PARAMS = pltpu.CompilerParams(vmem_limit_bytes=16 << 20)


def tables(size):
    freq = np.arange(GROUP)[:, None]
    place = np.arange(GROUP)[None, :]
    factor = np.where(freq == 0, np.sqrt(1.0 / GROUP), np.sqrt(2.0 / GROUP))
    table = factor * np.cos(np.pi * (2.0 * place + 1.0) * freq / (2.0 * GROUP))
    table = np.kron(np.eye(size // GROUP), table)
    high = table.astype(jnp.bfloat16)
    low = (table - high.astype(np.float64)).astype(jnp.bfloat16)
    return jnp.asarray(np.stack([high, low, high.T, low.T]))


def vmem(value):
    return pltpu.with_memory_space_constraint(value, pltpu.VMEM)


def left_table(high, low):
    return jnp.concatenate(
        [jnp.concatenate([high, high], 1), jnp.concatenate([low, low], 1)], 0
    )


def right_table(high, low):
    row = jnp.concatenate([high, low], 1)
    return jnp.concatenate([row, row], 0)


def split(value, axis):
    high = value.astype(BF16)
    low = (value - high.astype(F32)).astype(BF16)
    return jnp.concatenate([high, low], axis=axis)


def mm(a, b):
    return jnp.dot(a, b, preferred_element_type=F32)


def mm_t(a, b):
    return lax.dot_general(a, b, (((0,), (0,)), ((), ())), preferred_element_type=F32)


def add_columns(both):
    half = both.shape[1] // 2
    return both[:, :half] + both[:, half:]


def right(value, table):
    return add_columns(mm(split(value, 1), table))


def left(table, value):
    both = mm(table, split(value, 0))
    half = both.shape[0] // 2
    return both[:half] + both[half:]


def forward_kernel(
    inner, select, x_hbm, g, m_hbm, dct, *refs
):
    picks, rest = refs[:inner], refs[inner]
    x, m, c1, f2, listed, index_v, index, sems, sel_sem = refs[inner + 1 :]
    me = lax.axis_index("dp")
    rows, cols = m.shape
    steps, slots, owners = index.shape
    per_class = owners // inner
    mine = me % inner
    fetch = pltpu.make_async_copy(select.at[me], listed, sel_sem)
    fetch.start()
    width = rows // CHUNKS
    copies = []
    for c in range(CHUNKS):
        span = pl.ds(c * width, width)
        a = pltpu.make_async_copy(x_hbm.at[:, :, span], x.at[:, :, span], sems.at[c, 0])
        b = pltpu.make_async_copy(m_hbm.at[span], m.at[span], sems.at[c, 1])
        a.start()
        b.start()
        copies.append((a, b))
    c1[pl.ds(rows, 8), :] = jnp.zeros((8, cols), F32)
    rest[pl.ds(rows, 8), :] = jnp.zeros((8, cols), F32)
    table = right_table(dct[2], dct[3])
    row_table = left_table(dct[0], dct[1])
    second = split(add_columns(mm(g[1], table[:cols])), 1)
    first = g[0]
    fetch.wait()
    owner = lax.broadcasted_iota(jnp.int32, listed.shape, 2)
    index_v[...] = jnp.where(listed[...] >= 0, listed[...] + owner * (rows // owners), rows)
    store = pltpu.make_async_copy(index_v, index, sel_sem)
    store.start()
    for c in range(CHUNKS):
        copies[c][0].wait()
        copies[c][1].wait()
        for r in range(c * width, (c + 1) * width, cols):
            m1 = 0.999 * m[r : r + cols] + mm_t(x[0, :, r : r + cols], first)
            y1 = right(m1, table)
            y2 = add_columns(mm_t(x[1, :, r : r + cols], second))
            z = left(row_table, jnp.concatenate([y1, y2], axis=1))
            c1[r : r + cols] = z[:, :cols]
            f2[r : r + cols] = z[:, cols:]
    store.wait()
    zero = jnp.zeros((1, cols), F32)

    def gather(step, source):
        for j in range(inner):
            base = (mine ^ j) * per_class
            for k in range(per_class):
                for c in range(slots):
                    place = (k * steps + step) * slots + c
                    picks[j][pl.ds(place, 1), :] = source[pl.ds(index[step, c, base + k], 1), :]

    def clear(step, target):
        for k in range(owners):
            for c in range(slots):
                target[pl.ds(index[step, c, k], 1), :] = zero

    gather(0, c1)
    clear(0, c1)
    rest[:rows] = 0.999 * c1[:rows] + f2[...]
    gather(1, rest)
    clear(1, rest)


def forward(select, x, g, m, dct, inner):
    rows, cols = m.shape
    steps = x.shape[0]
    owners, _, slots, _ = select.shape
    block = pltpu.VMEM((owners // inner * steps * slots, cols), F32)
    return pl.pallas_call(
        functools.partial(forward_kernel, inner),
        out_shape=[block] * inner + [pltpu.VMEM((rows + 8, cols), F32)],
        in_specs=[IN_HBM, IN_HBM, IN_VMEM, IN_HBM, IN_VMEM],
        out_specs=[IN_VMEM] * (inner + 1),
        scratch_shapes=[
            pltpu.VMEM(x.shape, x.dtype),
            pltpu.VMEM((rows, cols), F32),
            pltpu.VMEM((rows + 8, cols), F32),
            pltpu.VMEM((rows, cols), F32),
            pltpu.VMEM(select.shape[1:], jnp.int32),
            pltpu.VMEM(select.shape[1:], jnp.int32),
            pltpu.SMEM(select.shape[1:], jnp.int32),
            pltpu.SemaphoreType.DMA((CHUNKS, 2)),
            pltpu.SemaphoreType.DMA,
        ],
        compiler_params=PARAMS,
        name="forward",
    )(select, x, g, m, dct)


def inverse_tile(value, row_table, col_table):
    return left(row_table, right(value, col_table))


def inverse_kernel(coeffs, dct, out):
    row_table, table = left_table(dct[2], dct[3]), right_table(dct[0], dct[1])
    rows, cols = out.shape
    for r in range(0, rows, cols):
        out[r : r + cols] = inverse_tile(coeffs[r : r + cols], row_table, table)


def inverse(coeffs, dct, rows):
    cols = coeffs.shape[1]
    return pl.pallas_call(
        inverse_kernel,
        out_shape=jax.ShapeDtypeStruct((rows, cols), F32),
        in_specs=[IN_VMEM] * 2,
        out_specs=IN_VMEM,
        compiler_params=PARAMS,
        name="inverse",
    )(vmem(coeffs), dct)


def class_kernel(inner, listed, dct, *refs):
    blocks, out, ordered, total = refs[:-3], refs[-3], refs[-2], refs[-1]
    me = lax.axis_index("dp")
    rows, cols = out.shape
    per_class, slots = listed.shape
    per_owner = rows // per_class
    replicas = len(blocks) * inner
    each = slots // replicas
    for k, block in enumerate(blocks):
        for j in range(inner):
            replica = (me // inner ^ k) * inner + (me % inner ^ j)
            span = pl.ds(pl.multiple_of(replica * each, each), each)
            for o in range(per_class):
                ordered[o, span, :] = split(block[pl.ds((j * per_class + o) * each, each), :], 1)
    ids = lax.broadcasted_iota(jnp.int32, (per_owner, slots), 0)
    for o in range(per_class):
        onehot = jnp.where(ids == listed[pl.ds(o, 1), :], 1.0, 0.0).astype(BF16)
        total[pl.ds(o * per_owner, per_owner), :] = add_columns(mm(onehot, ordered[o]))
    row_table, table = left_table(dct[2], dct[3]), right_table(dct[0], dct[1])
    for r in range(0, rows, cols):
        out[r : r + cols] = inverse_tile(total[r : r + cols], row_table, table)


def class_rows(listed, blocks, dct, inner, rows):
    cols = blocks[0].shape[1]
    per_class, slots = listed.shape
    return pl.pallas_call(
        functools.partial(class_kernel, inner),
        out_shape=pltpu.VMEM((rows, cols), F32),
        in_specs=[IN_VMEM] * (2 + len(blocks)),
        out_specs=IN_VMEM,
        scratch_shapes=[
            pltpu.VMEM((per_class, slots, 2 * cols), BF16),
            pltpu.VMEM((rows, cols), F32),
        ],
        compiler_params=PARAMS,
        name="class_rows",
    )(listed, dct, *[vmem(b) for b in blocks])


def finish_kernel(*refs):
    count = len(refs) // 2
    blocks, out, held, sems = refs[:-3], refs[-3], refs[-2], refs[-1]
    me = lax.axis_index("dp")
    copies = []
    for j, block in enumerate(blocks):
        held[j] = block[...].astype(held.dtype)
        copy = pltpu.make_async_copy(held.at[j], out.at[me % len(blocks) ^ j], sems.at[j])
        copy.start()
        copies.append(copy)
    for copy in copies:
        copy.wait()


def finish(blocks):
    shape = (len(blocks),) + blocks[0].shape
    return pl.pallas_call(
        finish_kernel,
        out_shape=jax.ShapeDtypeStruct(shape, BF16),
        in_specs=[IN_VMEM] * len(blocks),
        out_specs=IN_HBM,
        scratch_shapes=[pltpu.VMEM(shape, BF16), pltpu.SemaphoreType.DMA((len(blocks),))],
        compiler_params=PARAMS,
        name="finish",
    )(*[vmem(b) for b in blocks])


def per_device(inputs, grad_out, momentum, select):
    replica = lax.axis_index("dp")
    owners = lax.axis_size("dp")
    rows, cols = momentum.shape[1:]
    inner = 1
    while inner * inner < owners:
        inner *= 2
    outer = owners // inner
    dct = tables(cols)

    def from_peer(value, shift):
        return lax.ppermute(value, "dp", [(d, d ^ shift) for d in range(owners)])

    *picks, rest = forward(
        jnp.swapaxes(select, 2, 3), inputs[0], grad_out[0], momentum[0], dct, inner
    )
    plane = jnp.concatenate(
        [picks[0]] + [from_peer(picks[j], j) for j in range(1, inner)]
    )
    blocks = [plane] + [from_peer(plane, k * inner) for k in range(1, outer)]
    new_momentum = inverse(rest, dct, rows)
    listed = jnp.transpose(select, (2, 0, 1, 3)).reshape(owners, -1)
    listed = lax.dynamic_slice_in_dim(listed, replica % inner * outer, outer, 0)
    own = class_rows(listed, blocks, dct, inner, rows // inner)
    update = finish([own] + [from_peer(own, j) for j in range(1, inner)])
    return (update.reshape(rows, cols), new_momentum[None])


def solution(mesh):
    return jax.shard_map(
        per_device,
        mesh=mesh,
        in_specs=(
            P("dp", None, None, None),
            P("dp", None, None, "mp"),
            P("dp", None, "mp"),
            P(None, None, None, "mp"),
        ),
        out_specs=(P(None, "mp"), P("dp", None, "mp")),
        check_vma=False,
    )
```

```python
import functools

import jax
import jax.numpy as jnp
import numpy as np
from jax import lax
from jax.experimental import pallas as pl
from jax.experimental.pallas import tpu as pltpu
from jax.sharding import PartitionSpec as P

GROUP = 64
CHUNKS = 2
F32 = jnp.float32
BF16 = jnp.bfloat16
IN_VMEM = pl.BlockSpec(memory_space=pltpu.VMEM)
IN_HBM = pl.BlockSpec(memory_space=pltpu.HBM)
PARAMS = pltpu.CompilerParams(vmem_limit_bytes=16 << 20)


def tables(size):
    freq = np.arange(GROUP)[:, None]
    place = np.arange(GROUP)[None, :]
    factor = np.where(freq == 0, np.sqrt(1.0 / GROUP), np.sqrt(2.0 / GROUP))
    table = factor * np.cos(np.pi * (2.0 * place + 1.0) * freq / (2.0 * GROUP))
    table = np.kron(np.eye(size // GROUP), table)
    high = table.astype(jnp.bfloat16)
    low = (table - high.astype(np.float64)).astype(jnp.bfloat16)
    return jnp.asarray(np.stack([high, low, high.T, low.T]))


def vmem(value):
    return pltpu.with_memory_space_constraint(value, pltpu.VMEM)


def hbm(value):
    return pltpu.with_memory_space_constraint(value, pltpu.HBM)


def left_table(high, low):
    return jnp.concatenate(
        [jnp.concatenate([high, high], 1), jnp.concatenate([low, low], 1)], 0
    )


def right_table(high, low):
    row = jnp.concatenate([high, low], 1)
    return jnp.concatenate([row, row], 0)


def split(value, axis):
    high = value.astype(BF16)
    low = (value - high.astype(F32)).astype(BF16)
    return jnp.concatenate([high, low], axis=axis)


def mm(a, b):
    return jnp.dot(a, b, preferred_element_type=F32)


def mm_nt(a, b):
    return lax.dot_general(a, b, (((1,), (1,)), ((), ())), preferred_element_type=F32)


def add_columns(both):
    half = both.shape[1] // 2
    return both[:, :half] + both[:, half:]


def add_rows(both):
    half = both.shape[0] // 2
    return both[:half] + both[half:]


def right(value, table):
    return add_columns(mm(split(value, 1), table))


def left(table, value):
    return add_rows(mm(table, split(value, 0)))


def forward_kernel(inner, select, x_hbm, g_hbm, m_hbm, dct_hbm, *refs):
    picks, rest = refs[:inner], refs[inner]
    x, m, c1, f2, y, g, dct, listed, index_v, index, sems, small = refs[inner + 1 :]
    me = lax.axis_index("dp")
    rows, cols = m.shape
    steps, slots, owners = index.shape
    per_class = owners // inner
    mine = me % inner
    width = rows // CHUNKS

    def begin(source, target, sem):
        copy = pltpu.make_async_copy(source, target, sem)
        copy.start()
        return copy

    fetch_dct = begin(dct_hbm, dct, small.at[0])
    fetch_g = begin(g_hbm, g, small.at[1])
    fetch_select = begin(select.at[me], listed, small.at[2])
    for c in range(CHUNKS):
        span = pl.ds(c * width, width)
        begin(m_hbm.at[span], m.at[span], sems.at[c, 0])
        begin(x_hbm.at[:, :, span], x.at[:, :, span], sems.at[c, 1])
    c1[pl.ds(rows, 8), :] = jnp.zeros((8, cols), F32)
    rest[pl.ds(rows, 8), :] = jnp.zeros((8, cols), F32)
    fetch_dct.wait()
    table = left_table(dct[0], dct[1])
    fetch_g.wait()
    gradients = [split(add_rows(mm_nt(table[:, :cols], g[s])), 0) for s in range(steps)]
    fetch_select.wait()
    owner = lax.broadcasted_iota(jnp.int32, listed.shape, 2)
    index_v[...] = jnp.where(listed[...] >= 0, listed[...] + owner * (rows // owners), rows)
    store = begin(index_v, index, small.at[2])
    def arrive(c):
        span = pl.ds(c * width, width)
        pltpu.make_async_copy(m_hbm.at[span], m.at[span], sems.at[c, 0]).wait()
        pltpu.make_async_copy(x_hbm.at[:, :, span], x.at[:, :, span], sems.at[c, 1]).wait()

    def columns(c):
        span = pl.ds(c * width, width)
        y1 = 0.999 * add_rows(mm_nt(table, split(m[span, :], 1)))
        y1 = y1 + add_rows(mm(gradients[0], x[0, :, span]))
        y2 = add_rows(mm(gradients[1], x[1, :, span]))
        y[c % 2] = jnp.concatenate([y1, y2], axis=0)

    def transform(c):
        for t in range(0, width, cols):
            z = add_rows(mm_nt(table, split(y[c % 2, :, t : t + cols], 1)))
            span = pl.ds(c * width + t, cols)
            c1[span, :] = z[:, :cols]
            f2[span, :] = z[:, cols:]

    for c in range(CHUNKS):
        arrive(c)
        if c > 0:
            transform(c - 1)
        columns(c)
    transform(CHUNKS - 1)
    store.wait()
    zero = jnp.zeros((1, cols), F32)

    def gather(step, source):
        for j in range(inner):

            def one(k, _, j=j):
                base = (mine ^ j) * per_class
                for c in range(slots):
                    place = (k * steps + step) * slots + c
                    picks[j][pl.ds(place, 1), :] = source[pl.ds(index[step, c, base + k], 1), :]
                return 0

            for k in range(per_class):
                one(k, 0)

    def clear(step, target):
        def one(k, _):
            for c in range(slots):
                target[pl.ds(index[step, c, k], 1), :] = zero
            return 0

        for k in range(owners):
            one(k, 0)

    def second_step(c, _):
        span = pl.ds(pl.multiple_of(c * cols, cols), cols)
        rest[span, :] = 0.999 * c1[span, :] + f2[span, :]
        return 0

    gather(0, c1)
    clear(0, c1)
    rest[:rows] = 0.999 * c1[:rows] + f2[...]
    gather(1, rest)
    clear(1, rest)


def forward(select, x, g, m, dct, inner):
    rows, cols = m.shape
    steps = x.shape[0]
    owners, _, slots, _ = select.shape
    block = pltpu.VMEM((owners // inner * steps * slots, cols), F32)
    return pl.pallas_call(
        functools.partial(forward_kernel, inner),
        out_shape=[block] * inner + [pltpu.VMEM((rows + 8, cols), F32)],
        in_specs=[IN_HBM] * 5,
        out_specs=[IN_VMEM] * (inner + 1),
        scratch_shapes=[
            pltpu.VMEM(x.shape, x.dtype),
            pltpu.VMEM((rows, cols), F32),
            pltpu.VMEM((rows + 8, cols), F32),
            pltpu.VMEM((rows, cols), F32),
            pltpu.VMEM((2, steps * cols, rows // CHUNKS), F32),
            pltpu.VMEM(g.shape, g.dtype),
            pltpu.VMEM(dct.shape, dct.dtype),
            pltpu.VMEM(select.shape[1:], jnp.int32),
            pltpu.VMEM(select.shape[1:], jnp.int32),
            pltpu.SMEM(select.shape[1:], jnp.int32),
            pltpu.SemaphoreType.DMA((CHUNKS, 2)),
            pltpu.SemaphoreType.DMA((3,)),
        ],
        compiler_params=PARAMS,
        name="forward",
    )(hbm(select), hbm(x), hbm(g), hbm(m), hbm(dct))


def inverse_tile(value, row_table, col_table):
    return left(row_table, right(value, col_table))


def invert(source, target, row_table, table):
    rows, cols = target.shape

    def pair(c, _):
        for t in range(2):
            span = pl.ds(pl.multiple_of((2 * c + t) * cols, cols), cols)
            target[span, :] = inverse_tile(source[span, :], row_table, table)
        return 0

    lax.fori_loop(0, rows // (2 * cols), pair, 0)


def inverse_kernel(coeffs, dct, out):
    row_table, table = left_table(dct[2], dct[3]), right_table(dct[0], dct[1])
    rows, cols = out.shape
    invert(coeffs, out, row_table, table)


def inverse(coeffs, dct, rows):
    cols = coeffs.shape[1]
    return pl.pallas_call(
        inverse_kernel,
        out_shape=jax.ShapeDtypeStruct((rows, cols), F32),
        in_specs=[IN_VMEM] * 2,
        out_specs=IN_VMEM,
        compiler_params=PARAMS,
        name="inverse",
    )(vmem(coeffs), dct)


def class_kernel(inner, listed, dct, *refs):
    blocks, out, ordered, total = refs[-4::-1], refs[-3], refs[-2], refs[-1]
    me = lax.axis_index("dp")
    rows, cols = out.shape
    per_class, slots = listed.shape
    per_owner = rows // per_class
    replicas = len(blocks) * inner
    each = slots // replicas
    for k, block in enumerate(blocks):
        for j in range(inner):
            replica = (me // inner ^ k) * inner + (me % inner ^ j)
            span = pl.ds(pl.multiple_of(replica * each, each), each)
            for o in range(per_class):
                ordered[o, span, :] = split(block[pl.ds((j * per_class + o) * each, each), :], 1)
    ids = lax.broadcasted_iota(jnp.int32, (per_owner, slots), 0)
    for o in range(per_class):
        onehot = jnp.where(ids == listed[pl.ds(o, 1), :], 1.0, 0.0).astype(BF16)
        total[pl.ds(o * per_owner, per_owner), :] = add_columns(mm(onehot, ordered[o]))
    row_table, table = left_table(dct[2], dct[3]), right_table(dct[0], dct[1])
    invert(total, out, row_table, table)


def class_rows(listed, blocks, dct, inner, rows):
    cols = blocks[0].shape[1]
    per_class, slots = listed.shape
    return pl.pallas_call(
        functools.partial(class_kernel, inner),
        out_shape=pltpu.VMEM((rows, cols), F32),
        in_specs=[IN_VMEM] * (2 + len(blocks)),
        out_specs=IN_VMEM,
        scratch_shapes=[
            pltpu.VMEM((per_class, slots, 2 * cols), BF16),
            pltpu.VMEM((rows, cols), F32),
        ],
        compiler_params=PARAMS,
        name="class_rows",
    )(listed, dct, *[vmem(b) for b in reversed(blocks)])


def finish_kernel(*refs):
    blocks, out, held, sems = refs[-4::-1], refs[-3], refs[-2], refs[-1]
    me = lax.axis_index("dp")
    copies = []
    for j, block in enumerate(blocks):
        held[j] = block[...].astype(held.dtype)
        copy = pltpu.make_async_copy(held.at[j], out.at[me % len(blocks) ^ j], sems.at[j])
        copy.start()
        copies.append(copy)
    for copy in copies:
        copy.wait()


def finish(blocks):
    shape = (len(blocks),) + blocks[0].shape
    return pl.pallas_call(
        finish_kernel,
        out_shape=jax.ShapeDtypeStruct(shape, BF16),
        in_specs=[IN_VMEM] * len(blocks),
        out_specs=IN_HBM,
        scratch_shapes=[pltpu.VMEM(shape, BF16), pltpu.SemaphoreType.DMA((len(blocks),))],
        compiler_params=PARAMS,
        name="finish",
    )(*[vmem(b) for b in reversed(blocks)])


def per_device(inputs, grad_out, momentum, select):
    replica = lax.axis_index("dp")
    owners = lax.axis_size("dp")
    rows, cols = momentum.shape[1:]
    inner = 1
    while inner * inner < owners:
        inner *= 2
    outer = owners // inner
    dct = tables(cols)

    def from_peer(value, shift):
        return lax.ppermute(value, "dp", [(d, d ^ shift) for d in range(owners)])

    def from_peers(values, stride):
        return [values[0]] + [
            from_peer(values[j], j * stride) for j in range(1, len(values))
        ]

    *picks, rest = forward(
        jnp.swapaxes(select, 2, 3), inputs[0], grad_out[0], momentum[0], dct, inner
    )
    plane = jnp.concatenate(from_peers(picks, 1))
    blocks = from_peers([plane] * outer, inner)
    new_momentum = inverse(rest, dct, rows)
    listed = jnp.transpose(select, (2, 0, 1, 3)).reshape(owners, -1)
    listed = lax.dynamic_slice_in_dim(listed, replica % inner * outer, outer, 0)
    own = class_rows(listed, blocks, dct, inner, rows // inner)
    update = finish(from_peers([own] * inner, 1))
    return (update.reshape(rows, cols), new_momentum[None])


def solution(mesh):
    return jax.shard_map(
        per_device,
        mesh=mesh,
        in_specs=(
            P("dp", None, None, None),
            P("dp", None, None, "mp"),
            P("dp", None, "mp"),
            P(None, None, None, "mp"),
        ),
        out_specs=(P(None, "mp"), P("dp", None, "mp")),
        check_vma=False,
    )
```

```python
import functools

import jax
import jax.numpy as jnp
import numpy as np
from jax import lax
from jax.experimental import pallas as pl
from jax.experimental.pallas import tpu as pltpu
from jax.sharding import PartitionSpec as P


GROUP = 64
CHUNKS = 2
HALVES = 2
F32 = jnp.float32
BF16 = jnp.bfloat16
IN_VMEM = pl.BlockSpec(memory_space=pltpu.VMEM)
IN_HBM = pl.BlockSpec(memory_space=pltpu.HBM)
PARAMS = pltpu.CompilerParams(vmem_limit_bytes=16 << 20)


def tables(size):
    freq = np.arange(GROUP)[:, None]
    place = np.arange(GROUP)[None, :]
    factor = np.where(freq == 0, np.sqrt(1.0 / GROUP), np.sqrt(2.0 / GROUP))
    table = factor * np.cos(np.pi * (2.0 * place + 1.0) * freq / (2.0 * GROUP))
    table = np.kron(np.eye(size // GROUP), table)
    high = table.astype(jnp.bfloat16)
    low = (table - high.astype(np.float64)).astype(jnp.bfloat16)
    return jnp.asarray(np.stack([high, low, high.T, low.T]))


def vmem(value):
    return pltpu.with_memory_space_constraint(value, pltpu.VMEM)


def hbm(value):
    return pltpu.with_memory_space_constraint(value, pltpu.HBM)


def left_table(high, low):
    return jnp.concatenate(
        [jnp.concatenate([high, high], 1), jnp.concatenate([low, low], 1)], 0
    )


def right_table(high, low):
    row = jnp.concatenate([high, low], 1)
    return jnp.concatenate([row, row], 0)


def split(value, axis):
    high = value.astype(BF16)
    low = (value - high.astype(F32)).astype(BF16)
    return jnp.concatenate([high, low], axis=axis)


def mm(a, b):
    return jnp.dot(a, b, preferred_element_type=F32)


def mm_nt(a, b):
    return lax.dot_general(a, b, (((1,), (1,)), ((), ())), preferred_element_type=F32)


def add_columns(both):
    half = both.shape[1] // 2
    return both[:, :half] + both[:, half:]


def add_rows(both):
    half = both.shape[0] // 2
    return both[:half] + both[half:]


def right(value, table):
    return add_columns(mm(split(value, 1), table))


def left(table, value):
    return add_rows(mm(table, split(value, 0)))


def forward_kernel(inner, select, x_hbm, g_hbm, m_hbm, dct_hbm, *refs):
    picks, rest = refs[:inner], refs[inner]
    x, m, c1, f2, y, g, dct, listed, index_v, index, sems, small = refs[inner + 1 :]
    me = lax.axis_index("dp")
    rows, cols = m.shape
    steps, slots, owners = index.shape
    per_class = owners // inner
    mine = me % inner
    width = rows // CHUNKS

    def begin(source, target, sem):
        copy = pltpu.make_async_copy(source, target, sem)
        copy.start()
        return copy

    fetch_dct = begin(dct_hbm, dct, small.at[0])
    fetch_g = begin(g_hbm, g, small.at[1])
    fetch_select = begin(select.at[me], listed, small.at[2])
    for c in range(CHUNKS):
        span = pl.ds(c * width, width)
        begin(m_hbm.at[span], m.at[span], sems.at[c, 0])
        begin(x_hbm.at[:, :, span], x.at[:, :, span], sems.at[c, 1])
    c1[pl.ds(rows, 8), :] = jnp.zeros((8, cols), F32)
    rest[pl.ds(rows, 8), :] = jnp.zeros((8, cols), F32)
    fetch_dct.wait()
    table = left_table(dct[0], dct[1])
    fetch_g.wait()
    gradients = [split(add_rows(mm_nt(table[:, :cols], g[s])), 0) for s in range(steps)]
    fetch_select.wait()
    owner = lax.broadcasted_iota(jnp.int32, listed.shape, 2)
    index_v[...] = jnp.where(listed[...] >= 0, listed[...] + owner * (rows // owners), rows)
    store = begin(index_v, index, small.at[2])

    def arrive(c):
        span = pl.ds(c * width, width)
        pltpu.make_async_copy(m_hbm.at[span], m.at[span], sems.at[c, 0]).wait()
        pltpu.make_async_copy(x_hbm.at[:, :, span], x.at[:, :, span], sems.at[c, 1]).wait()

    def columns(c):
        span = pl.ds(c * width, width)
        y1 = 0.999 * add_rows(mm_nt(table, split(m[span, :], 1)))
        y1 = y1 + add_rows(mm(gradients[0], x[0, :, span]))
        y2 = add_rows(mm(gradients[1], x[1, :, span]))
        y[c % 2] = jnp.concatenate([y1, y2], axis=0)

    def transform(c):
        for t in range(0, width, cols):
            z = add_rows(mm_nt(table, split(y[c % 2, :, t : t + cols], 1)))
            span = pl.ds(c * width + t, cols)
            c1[span, :] = z[:, :cols]
            f2[span, :] = z[:, cols:]

    for c in range(CHUNKS):
        arrive(c)
        if c > 0:
            transform(c - 1)
        columns(c)
    transform(CHUNKS - 1)
    store.wait()
    zero = jnp.zeros((1, cols), F32)

    def gather(step, source):
        for j in range(inner):

            def one(k, j=j):
                base = (mine ^ j) * per_class
                for c in range(slots):
                    place = (k * steps + step) * slots + c
                    picks[j][pl.ds(place, 1), :] = source[pl.ds(index[step, c, base + k], 1), :]
                return 0

            for k in range(per_class):
                one(k)

    def clear(step, target):
        def one(k):
            for c in range(slots):
                target[pl.ds(index[step, c, k], 1), :] = zero
            return 0

        for k in range(owners):
            one(k)

    gather(0, c1)
    clear(0, c1)
    rest[:rows] = 0.999 * c1[:rows] + f2[...]
    gather(1, rest)
    clear(1, rest)


def forward(select, x, g, m, dct, inner):
    rows, cols = m.shape
    steps = x.shape[0]
    owners, _, slots, _ = select.shape
    block = pltpu.VMEM((owners // inner * steps * slots, cols), F32)
    return pl.pallas_call(
        functools.partial(forward_kernel, inner),
        out_shape=[block] * inner + [pltpu.VMEM((rows + 8, cols), F32)],
        in_specs=[IN_HBM] * 5,
        out_specs=[IN_VMEM] * (inner + 1),
        scratch_shapes=[
            pltpu.VMEM(x.shape, x.dtype),
            pltpu.VMEM((rows, cols), F32),
            pltpu.VMEM((rows + 8, cols), F32),
            pltpu.VMEM((rows, cols), F32),
            pltpu.VMEM((2, steps * cols, rows // CHUNKS), F32),
            pltpu.VMEM(g.shape, g.dtype),
            pltpu.VMEM(dct.shape, dct.dtype),
            pltpu.VMEM(select.shape[1:], jnp.int32),
            pltpu.VMEM(select.shape[1:], jnp.int32),
            pltpu.SMEM(select.shape[1:], jnp.int32),
            pltpu.SemaphoreType.DMA((CHUNKS, 2)),
            pltpu.SemaphoreType.DMA((3,)),
        ],
        compiler_params=PARAMS,
        name="forward",
    )(hbm(select), hbm(x), hbm(g), hbm(m), hbm(dct))


def inverse_tile(value, row_table, col_table):
    return left(row_table, right(value, col_table))


def invert(source, target, row_table, table):
    rows, cols = target.shape

    def pair(c):
        for t in range(2):
            span = pl.ds((2 * c + t) * cols, cols)
            target[span, :] = inverse_tile(source[span, :], row_table, table)
        return 0

    for c in range(rows // (2 * cols)):
        pair(c)


def inverse_kernel(coeffs, dct, out):
    row_table, table = left_table(dct[2], dct[3]), right_table(dct[0], dct[1])
    invert(coeffs, out, row_table, table)


def inverse(coeffs, dct, rows):
    cols = coeffs.shape[1]
    return pl.pallas_call(
        inverse_kernel,
        out_shape=jax.ShapeDtypeStruct((rows, cols), F32),
        in_specs=[IN_VMEM] * 2,
        out_specs=IN_VMEM,
        compiler_params=PARAMS,
        name="inverse",
    )(vmem(coeffs), dct)


def class_kernel(inner, listed, dct, *refs):
    blocks, out, ordered, total = refs[-4::-1], refs[-3], refs[-2], refs[-1]
    me = lax.axis_index("dp")
    rows, cols = out.shape
    per_class, slots = listed.shape
    per_owner = rows // per_class
    replicas = len(blocks) * inner
    each = slots // replicas
    for k, block in enumerate(blocks):
        for j in range(inner):
            replica = (me // inner ^ k) * inner + (me % inner ^ j)
            span = pl.ds(pl.multiple_of(replica * each, each), each)
            for o in range(per_class):
                ordered[o, span, :] = split(block[pl.ds((j * per_class + o) * each, each), :], 1)
    ids = lax.broadcasted_iota(jnp.int32, (per_owner, slots), 0)
    for o in range(per_class):
        onehot = jnp.where(ids == listed[pl.ds(o, 1), :], 1.0, 0.0).astype(BF16)
        total[pl.ds(o * per_owner, per_owner), :] = add_columns(mm(onehot, ordered[o]))
    row_table, table = left_table(dct[2], dct[3]), right_table(dct[0], dct[1])
    for r in range(0, rows, cols):
        out[r : r + cols] = inverse_tile(total[r : r + cols], row_table, table)


def class_rows(listed, blocks, dct, inner, rows):
    cols = blocks[0].shape[1]
    per_class, slots = listed.shape
    return pl.pallas_call(
        functools.partial(class_kernel, inner),
        out_shape=pltpu.VMEM((rows, cols), F32),
        in_specs=[IN_VMEM] * (2 + len(blocks)),
        out_specs=IN_VMEM,
        scratch_shapes=[
            pltpu.VMEM((per_class, slots, 2 * cols), BF16),
            pltpu.VMEM((rows, cols), F32),
        ],
        compiler_params=PARAMS,
        name="class_rows",
    )(listed, dct, *[vmem(b) for b in reversed(blocks)])


def finish_kernel(halves, *refs):
    blocks, out, held, sems = refs[-4::-1], refs[-3], refs[-2], refs[-1]
    me = lax.axis_index("dp")
    inner = len(blocks) // halves
    copies = []
    for h in range(halves):
        for j in range(inner):
            i = h * inner + j
            held[i] = blocks[i][...].astype(held.dtype)
            copy = pltpu.make_async_copy(held.at[i], out.at[me % inner ^ j, h], sems.at[i])
            copy.start()
            copies.append(copy)
    for copy in copies:
        copy.wait()


def finish(outs):
    blocks = [b for half in outs for b in half]
    shape = blocks[0].shape
    return pl.pallas_call(
        functools.partial(finish_kernel, len(outs)),
        out_shape=jax.ShapeDtypeStruct((len(outs[0]), len(outs)) + shape, BF16),
        in_specs=[IN_VMEM] * len(blocks),
        out_specs=IN_HBM,
        scratch_shapes=[
            pltpu.VMEM((len(blocks),) + shape, BF16),
            pltpu.SemaphoreType.DMA((len(blocks),)),
        ],
        compiler_params=PARAMS,
        name="finish",
    )(*[vmem(b) for b in reversed(blocks)])


def inner_size(owners):
    inner = 1
    while inner * inner < owners:
        inner *= 2
    return inner


def per_device(inputs, grad_out, momentum, select):
    replica = lax.axis_index("dp")
    owners = lax.axis_size("dp")
    rows, cols = momentum.shape[1:]
    inner = inner_size(owners)
    outer = owners // inner
    dct = tables(cols)

    def from_peer(value, shift):
        return lax.ppermute(value, "dp", [(d, d ^ shift) for d in range(owners)])

    def from_peers(values, stride):
        got = [values[0]]
        for j in range(1, len(values)):
            got.append(from_peer(values[j], j * stride))
        return got

    *picks, rest = forward(
        jnp.swapaxes(select, 2, 3), inputs[0], grad_out[0], momentum[0], dct, inner
    )
    listed = jnp.transpose(select, (2, 0, 1, 3)).reshape(owners, -1)
    listed = lax.dynamic_slice_in_dim(listed, replica % inner * outer, outer, 0)
    peers = from_peers(picks, 1)
    each = owners // inner // HALVES
    lines, outs = [], []
    for h in range(HALVES):
        span = slice(h * picks[0].shape[0] // HALVES, (h + 1) * picks[0].shape[0] // HALVES)
        plane = jnp.concatenate([p[span] for p in peers])
        lines.append(from_peers([plane] * outer, inner))
    for h in range(HALVES):
        own = class_rows(
            listed[h * each : (h + 1) * each], lines[h], dct, inner, rows // inner // HALVES
        )
        outs.append(from_peers([own] * inner, 1))
    new_momentum = inverse(rest, dct, rows)
    update = finish(outs)
    return (update.reshape(rows, cols), new_momentum[None])


def solution(mesh):
    return jax.shard_map(
        per_device,
        mesh=mesh,
        in_specs=(
            P("dp", None, None, None),
            P("dp", None, None, "mp"),
            P("dp", None, "mp"),
            P(None, None, None, "mp"),
        ),
        out_specs=(P(None, "mp"), P("dp", None, "mp")),
        check_vma=False,
    )
```

```python
import functools

import jax
import jax.numpy as jnp
import numpy as np
from jax import lax
from jax.experimental import pallas as pl
from jax.experimental.pallas import tpu as pltpu
from jax.sharding import PartitionSpec as P


GROUP = 64
CHUNKS = 2
HALVES = 2
F32 = jnp.float32
BF16 = jnp.bfloat16
IN_VMEM = pl.BlockSpec(memory_space=pltpu.VMEM)
IN_HBM = pl.BlockSpec(memory_space=pltpu.HBM)
PARAMS = pltpu.CompilerParams(vmem_limit_bytes=16 << 20)


def tables(size):
    freq = np.arange(GROUP)[:, None]
    place = np.arange(GROUP)[None, :]
    factor = np.where(freq == 0, np.sqrt(1.0 / GROUP), np.sqrt(2.0 / GROUP))
    table = factor * np.cos(np.pi * (2.0 * place + 1.0) * freq / (2.0 * GROUP))
    table = np.kron(np.eye(size // GROUP), table)
    high = table.astype(jnp.bfloat16)
    low = (table - high.astype(np.float64)).astype(jnp.bfloat16)
    return jnp.asarray(np.stack([high, low, high.T, low.T]))


def vmem(value):
    return pltpu.with_memory_space_constraint(value, pltpu.VMEM)


def hbm(value):
    return pltpu.with_memory_space_constraint(value, pltpu.HBM)


def left_table(high, low):
    return jnp.concatenate(
        [jnp.concatenate([high, high], 1), jnp.concatenate([low, low], 1)], 0
    )


def right_table(high, low):
    row = jnp.concatenate([high, low], 1)
    return jnp.concatenate([row, row], 0)


def split(value, axis):
    high = value.astype(BF16)
    low = (value - high.astype(F32)).astype(BF16)
    return jnp.concatenate([high, low], axis=axis)


def mm(a, b):
    return jnp.dot(a, b, preferred_element_type=F32)


def mm_nt(a, b):
    return lax.dot_general(a, b, (((1,), (1,)), ((), ())), preferred_element_type=F32)


def add_columns(both):
    half = both.shape[1] // 2
    return both[:, :half] + both[:, half:]


def add_rows(both):
    half = both.shape[0] // 2
    return both[:half] + both[half:]


def right(value, table):
    return add_columns(mm(split(value, 1), table))


def left(table, value):
    return add_rows(mm(table, split(value, 0)))


def forward_kernel(inner, select, x_hbm, g_hbm, m_hbm, dct_hbm, *refs):
    picks, rest = refs[:inner], refs[inner : inner + CHUNKS]
    scratch = refs[inner + CHUNKS :]
    c1, f2, scratch = scratch[:CHUNKS], scratch[CHUNKS : 2 * CHUNKS], scratch[2 * CHUNKS :]
    x, m, y, chosen, g, dct, listed, index_v, index, sems, small = scratch
    me = lax.axis_index("dp")
    rows, cols = m.shape
    steps, slots, owners = index.shape
    per_class = owners // inner
    width = rows // CHUNKS
    owned = owners // CHUNKS

    def begin(source, target, sem):
        copy = pltpu.make_async_copy(source, target, sem)
        copy.start()
        return copy

    fetch_dct = begin(dct_hbm, dct, small.at[0])
    fetch_g = begin(g_hbm, g, small.at[1])
    fetch_select = begin(select.at[me], listed, small.at[2])
    for c in range(CHUNKS):
        span = pl.ds(c * width, width)
        begin(m_hbm.at[span], m.at[span], sems.at[c, 0])
        begin(x_hbm.at[:, :, span], x.at[:, :, span], sems.at[c, 1])
    zero = jnp.zeros((1, cols), F32)
    for c in range(CHUNKS):
        c1[c][pl.ds(width, 8), :] = jnp.zeros((8, cols), F32)
        rest[c][pl.ds(width, 8), :] = jnp.zeros((8, cols), F32)
    fetch_dct.wait()
    table = left_table(dct[0], dct[1])
    fetch_g.wait()
    gradients = [split(add_rows(mm_nt(table[:, :cols], g[s])), 0) for s in range(steps)]
    fetch_select.wait()
    owner = lax.broadcasted_iota(jnp.int32, listed.shape, 2) % owned
    index_v[...] = jnp.where(listed[...] >= 0, listed[...] + owner * (rows // owners), width)
    store = begin(index_v, index, small.at[2])

    def arrive(c):
        span = pl.ds(c * width, width)
        pltpu.make_async_copy(m_hbm.at[span], m.at[span], sems.at[c, 0]).wait()
        pltpu.make_async_copy(x_hbm.at[:, :, span], x.at[:, :, span], sems.at[c, 1]).wait()

    def columns(c):
        span = pl.ds(c * width, width)
        y1 = 0.999 * add_rows(mm_nt(table, split(m[span, :], 1)))
        y1 = y1 + add_rows(mm(gradients[0], x[0, :, span]))
        y2 = add_rows(mm(gradients[1], x[1, :, span]))
        y[c % 2] = jnp.concatenate([y1, y2], axis=0)

    def transform(c):
        for t in range(0, width, cols):
            z = add_rows(mm_nt(table, split(y[c % 2, :, t : t + cols], 1)))
            c1[c][t : t + cols] = z[:, :cols]
            f2[c][t : t + cols] = z[:, cols:]

    def choose(c, step, source):
        for o in range(c * owned, (c + 1) * owned):
            for k in range(slots):
                chosen[o, pl.ds(step * slots + k, 1), :] = source[pl.ds(index[step, k, o], 1), :]

    def clear(c, step, target):
        for o in range(c * owned, (c + 1) * owned):
            for k in range(slots):
                target[pl.ds(index[step, k, o], 1), :] = zero

    def pick(c):
        choose(c, 0, c1[c])
        clear(c, 0, c1[c])
        rest[c][:width] = 0.999 * c1[c][:width] + f2[c][...]
        choose(c, 1, rest[c])
        clear(c, 1, rest[c])

    for c in range(CHUNKS):
        arrive(c)
        if c == CHUNKS - 1:
            store.wait()
        if c > 0:
            transform(c - 1)
        columns(c)
        if c > 0:
            pick(c - 1)
    transform(CHUNKS - 1)
    pick(CHUNKS - 1)
    for j in range(inner):
        own = chosen[pl.ds((me % inner ^ j) * per_class, per_class)]
        picks[j][...] = own.reshape(picks[j].shape)


def forward(select, x, g, m, dct, inner):
    rows, cols = m.shape
    steps = x.shape[0]
    owners, _, slots, _ = select.shape
    block = pltpu.VMEM((owners // inner * steps * slots, cols), F32)
    chunk = pltpu.VMEM((rows // CHUNKS + 8, cols), F32)
    return pl.pallas_call(
        functools.partial(forward_kernel, inner),
        out_shape=[block] * inner + [chunk] * CHUNKS,
        in_specs=[IN_HBM] * 5,
        out_specs=[IN_VMEM] * (inner + CHUNKS),
        scratch_shapes=[chunk] * CHUNKS
        + [pltpu.VMEM((rows // CHUNKS, cols), F32)] * CHUNKS
        + [
            pltpu.VMEM(x.shape, x.dtype),
            pltpu.VMEM((rows, cols), F32),
            pltpu.VMEM((2, steps * cols, rows // CHUNKS), F32),
            pltpu.VMEM((owners, steps * slots, cols), F32),
            pltpu.VMEM(g.shape, g.dtype),
            pltpu.VMEM(dct.shape, dct.dtype),
            pltpu.VMEM(select.shape[1:], jnp.int32),
            pltpu.VMEM(select.shape[1:], jnp.int32),
            pltpu.SMEM(select.shape[1:], jnp.int32),
            pltpu.SemaphoreType.DMA((CHUNKS, 2)),
            pltpu.SemaphoreType.DMA((3,)),
        ],
        compiler_params=PARAMS,
        name="forward",
    )(hbm(select), hbm(x), hbm(g), hbm(m), hbm(dct))


def inverse_tile(value, row_table, col_table):
    return left(row_table, right(value, col_table))


def inverse_kernel(dct, *refs):
    coeffs, (out, held, sems) = refs[:-3], refs[-3:]
    row_table, table = left_table(dct[2], dct[3]), right_table(dct[0], dct[1])
    rows, cols = out.shape
    width = rows // len(coeffs)
    part = rows // sems.shape[0]
    copies = []
    for r in range(0, rows, cols):
        source = coeffs[r // width]
        held[r : r + cols] = inverse_tile(
            source[r % width : r % width + cols], row_table, table
        )
        if (r + cols) % part == 0:
            span = pl.ds(r + cols - part, part)
            copy = pltpu.make_async_copy(held.at[span], out.at[span], sems.at[r // part])
            copy.start()
            copies.append(copy)
    for copy in copies:
        copy.wait()


def inverse(coeffs, dct, rows):
    cols = coeffs[0].shape[1]
    return pl.pallas_call(
        inverse_kernel,
        out_shape=jax.ShapeDtypeStruct((rows, cols), F32),
        in_specs=[IN_VMEM] * (1 + len(coeffs)),
        out_specs=IN_HBM,
        scratch_shapes=[pltpu.VMEM((rows, cols), F32), pltpu.SemaphoreType.DMA((4,))],
        compiler_params=PARAMS,
        name="inverse",
    )(dct, *[vmem(c) for c in coeffs])


def class_kernel(inner, listed, dct, *refs):
    blocks, out, ordered, total = refs[-4::-1], refs[-3], refs[-2], refs[-1]
    me = lax.axis_index("dp")
    rows, cols = out.shape
    per_class, slots = listed.shape
    per_owner = rows // per_class
    replicas = len(blocks) * inner
    each = slots // replicas
    for k, block in enumerate(blocks):
        for j in range(inner):
            replica = (me // inner ^ k) * inner + (me % inner ^ j)
            span = pl.ds(pl.multiple_of(replica * each, each), each)
            for o in range(per_class):
                ordered[o, span, :] = split(block[pl.ds((j * per_class + o) * each, each), :], 1)
    ids = lax.broadcasted_iota(jnp.int32, (per_owner, slots), 0)
    for o in range(per_class):
        onehot = jnp.where(ids == listed[pl.ds(o, 1), :], 1.0, 0.0).astype(BF16)
        total[pl.ds(o * per_owner, per_owner), :] = add_columns(mm(onehot, ordered[o]))
    row_table, table = left_table(dct[2], dct[3]), right_table(dct[0], dct[1])
    for r in range(0, rows, cols):
        out[r : r + cols] = inverse_tile(total[r : r + cols], row_table, table)


def class_rows(listed, blocks, dct, inner, rows):
    cols = blocks[0].shape[1]
    per_class, slots = listed.shape
    return pl.pallas_call(
        functools.partial(class_kernel, inner),
        out_shape=pltpu.VMEM((rows, cols), F32),
        in_specs=[IN_VMEM] * (2 + len(blocks)),
        out_specs=IN_VMEM,
        scratch_shapes=[
            pltpu.VMEM((per_class, slots, 2 * cols), BF16),
            pltpu.VMEM((rows, cols), F32),
        ],
        compiler_params=PARAMS,
        name="class_rows",
    )(listed, dct, *[vmem(b) for b in reversed(blocks)])


def finish_kernel(half, count, *refs):
    blocks, (out, held, sems) = refs[count - 1 :: -1], refs[-3:]
    me = lax.axis_index("dp")
    copies = []
    for j, block in enumerate(blocks):
        held[j] = block[...].astype(held.dtype)
        copy = pltpu.make_async_copy(held.at[j], out.at[me % count ^ j, half], sems.at[j])
        copy.start()
        copies.append(copy)
    for copy in copies:
        copy.wait()


def finish(half, blocks, earlier=None):
    kept = [] if earlier is None else [earlier]
    count, shape = len(blocks), blocks[0].shape
    return pl.pallas_call(
        functools.partial(finish_kernel, half, count),
        out_shape=jax.ShapeDtypeStruct((count, HALVES) + shape, BF16),
        in_specs=[IN_VMEM] * count + [IN_HBM] * len(kept),
        out_specs=IN_HBM,
        input_output_aliases={count: 0} if kept else {},
        scratch_shapes=[pltpu.VMEM((count,) + shape, BF16), pltpu.SemaphoreType.DMA((count,))],
        compiler_params=PARAMS,
        name="finish",
    )(*[vmem(b) for b in reversed(blocks)], *kept)


def inner_size(owners):
    inner = 1
    while inner * inner < owners:
        inner *= 2
    return inner


def per_device(inputs, grad_out, momentum, select):
    replica = lax.axis_index("dp")
    owners = lax.axis_size("dp")
    rows, cols = momentum.shape[1:]
    inner = inner_size(owners)
    outer = owners // inner
    dct = tables(cols)

    def from_peer(value, shift):
        return lax.ppermute(value, "dp", [(d, d ^ shift) for d in range(owners)])

    def from_peers(values, stride):
        got = [values[0]]
        for j in range(1, len(values)):
            got.append(from_peer(values[j], j * stride))
        return got

    made = forward(
        jnp.swapaxes(select, 2, 3), inputs[0], grad_out[0], momentum[0], dct, inner
    )
    picks, rest = made[:inner], made[inner:]
    listed = jnp.transpose(select, (2, 0, 1, 3)).reshape(owners, -1)
    listed = lax.dynamic_slice_in_dim(listed, replica % inner * outer, outer, 0)
    peers = from_peers(picks, 1)
    each = owners // inner // HALVES
    lines, outs = [], []
    for h in range(HALVES):
        span = slice(h * picks[0].shape[0] // HALVES, (h + 1) * picks[0].shape[0] // HALVES)
        plane = jnp.concatenate([p[span] for p in peers])
        lines.append(from_peers([plane] * outer, inner))
    for h in range(HALVES):
        own = class_rows(
            listed[h * each : (h + 1) * each], lines[h], dct, inner, rows // inner // HALVES
        )
        outs.append(from_peers([own] * inner, 1))
    new_momentum = inverse(rest, dct, rows)
    update = None
    for h, blocks in enumerate(outs):
        update = finish(h, blocks, update)
    return (update.reshape(rows, cols), new_momentum[None])


def solution(mesh):
    return jax.shard_map(
        per_device,
        mesh=mesh,
        in_specs=(
            P("dp", None, None, None),
            P("dp", None, None, "mp"),
            P("dp", None, "mp"),
            P(None, None, None, "mp"),
        ),
        out_specs=(P(None, "mp"), P("dp", None, "mp")),
        check_vma=False,
    )
```

```python
import functools

import jax
import jax.numpy as jnp
import numpy as np
from jax import lax
from jax.experimental import pallas as pl
from jax.experimental.pallas import tpu as pltpu
from jax.sharding import PartitionSpec as P


GROUP = 64
CHUNKS = 2
HALVES = 2
F32 = jnp.float32
BF16 = jnp.bfloat16
IN_VMEM = pl.BlockSpec(memory_space=pltpu.VMEM)
IN_HBM = pl.BlockSpec(memory_space=pltpu.HBM)
PARAMS = pltpu.CompilerParams(vmem_limit_bytes=16 << 20)


def tables(size):
    freq = np.arange(GROUP)[:, None]
    place = np.arange(GROUP)[None, :]
    factor = np.where(freq == 0, np.sqrt(1.0 / GROUP), np.sqrt(2.0 / GROUP))
    table = factor * np.cos(np.pi * (2.0 * place + 1.0) * freq / (2.0 * GROUP))
    table = np.kron(np.eye(size // GROUP), table)
    high = table.astype(jnp.bfloat16)
    low = (table - high.astype(np.float64)).astype(jnp.bfloat16)
    return jnp.asarray(np.stack([high, low, high.T, low.T]))


def vmem(value):
    return pltpu.with_memory_space_constraint(value, pltpu.VMEM)


def hbm(value):
    return pltpu.with_memory_space_constraint(value, pltpu.HBM)


def left_table(high, low):
    return jnp.concatenate(
        [jnp.concatenate([high, high], 1), jnp.concatenate([low, low], 1)], 0
    )


def right_table(high, low):
    row = jnp.concatenate([high, low], 1)
    return jnp.concatenate([row, row], 0)


def split(value, axis):
    high = value.astype(BF16)
    low = (value - high.astype(F32)).astype(BF16)
    return jnp.concatenate([high, low], axis=axis)


def mm(a, b):
    return jnp.dot(a, b, preferred_element_type=F32)


def mm_nt(a, b):
    return lax.dot_general(a, b, (((1,), (1,)), ((), ())), preferred_element_type=F32)


def add_columns(both):
    half = both.shape[1] // 2
    return both[:, :half] + both[:, half:]


def add_rows(both):
    half = both.shape[0] // 2
    return both[:half] + both[half:]


def right(value, table):
    return add_columns(mm(split(value, 1), table))


def left(table, value):
    return add_rows(mm(table, split(value, 0)))


def forward_kernel(inner, select, x_hbm, g_hbm, m_hbm, dct_hbm, *refs):
    picks, rest = refs[:inner], refs[inner : inner + CHUNKS]
    scratch = refs[inner + CHUNKS :]
    c1, f2, scratch = scratch[:CHUNKS], scratch[CHUNKS : 2 * CHUNKS], scratch[2 * CHUNKS :]
    x, m, y, chosen, g, dct, listed, index_v, index, sems, small = scratch
    me = lax.axis_index("dp")
    rows, cols = m.shape
    steps, slots, owners = index.shape
    per_class = owners // inner
    width = rows // CHUNKS
    owned = owners // CHUNKS

    def begin(source, target, sem):
        copy = pltpu.make_async_copy(source, target, sem)
        copy.start()
        return copy

    fetch_dct = begin(dct_hbm, dct, small.at[0])
    fetch_g = begin(g_hbm, g, small.at[1])
    fetch_select = begin(select.at[me], listed, small.at[2])
    for c in range(CHUNKS):
        span = pl.ds(c * width, width)
        begin(m_hbm.at[span], m.at[span], sems.at[c, 0])
        begin(x_hbm.at[:, :, span], x.at[:, :, span], sems.at[c, 1])
    zero = jnp.zeros((1, cols), F32)
    for c in range(CHUNKS):
        c1[c][pl.ds(width, 8), :] = jnp.zeros((8, cols), F32)
        rest[c][pl.ds(width, 8), :] = jnp.zeros((8, cols), F32)
    fetch_dct.wait()
    table = left_table(dct[0], dct[1])
    fetch_g.wait()
    gradients = [split(add_rows(mm_nt(table[:, :cols], g[s])), 0) for s in range(steps)]
    fetch_select.wait()
    owner = lax.broadcasted_iota(jnp.int32, listed.shape, 2) % owned
    index_v[...] = jnp.where(listed[...] >= 0, listed[...] + owner * (rows // owners), width)
    store = begin(index_v, index, small.at[2])

    def arrive(c):
        span = pl.ds(c * width, width)
        pltpu.make_async_copy(m_hbm.at[span], m.at[span], sems.at[c, 0]).wait()
        pltpu.make_async_copy(x_hbm.at[:, :, span], x.at[:, :, span], sems.at[c, 1]).wait()

    def columns(c):
        span = pl.ds(c * width, width)
        y1 = 0.999 * add_rows(mm_nt(table, split(m[span, :], 1)))
        y1 = y1 + add_rows(mm(gradients[0], x[0, :, span]))
        y2 = add_rows(mm(gradients[1], x[1, :, span]))
        y[c % 2] = jnp.concatenate([y1, y2], axis=0)

    def transform(c):
        for t in range(0, width, cols):
            z = add_rows(mm_nt(table, split(y[c % 2, :, t : t + cols], 1)))
            c1[c][t : t + cols] = z[:, :cols]
            f2[c][t : t + cols] = z[:, cols:]

    def choose(c, step, source):
        for o in range(c * owned, (c + 1) * owned):
            for k in range(slots):
                chosen[o, pl.ds(step * slots + k, 1), :] = source[pl.ds(index[step, k, o], 1), :]

    def clear(c, step, target):
        for o in range(c * owned, (c + 1) * owned):
            for k in range(slots):
                target[pl.ds(index[step, k, o], 1), :] = zero

    def pick(c):
        choose(c, 0, c1[c])
        clear(c, 0, c1[c])
        rest[c][:width] = 0.999 * c1[c][:width] + f2[c][...]
        choose(c, 1, rest[c])
        clear(c, 1, rest[c])

    for c in range(CHUNKS):
        arrive(c)
        if c == CHUNKS - 1:
            store.wait()
        if c > 0:
            transform(c - 1)
        columns(c)
        if c > 0:
            pick(c - 1)
    transform(CHUNKS - 1)
    pick(CHUNKS - 1)
    for j in range(inner):
        own = chosen[pl.ds((me % inner ^ j) * per_class, per_class)]
        picks[j][...] = own.reshape(picks[j].shape)


def forward(select, x, g, m, dct, inner):
    rows, cols = m.shape
    steps = x.shape[0]
    owners, _, slots, _ = select.shape
    block = pltpu.VMEM((owners // inner * steps * slots, cols), F32)
    chunk = pltpu.VMEM((rows // CHUNKS + 8, cols), F32)
    return pl.pallas_call(
        functools.partial(forward_kernel, inner),
        out_shape=[block] * inner + [chunk] * CHUNKS,
        in_specs=[IN_HBM] * 5,
        out_specs=[IN_VMEM] * (inner + CHUNKS),
        scratch_shapes=[chunk] * CHUNKS
        + [pltpu.VMEM((rows // CHUNKS, cols), F32)] * CHUNKS
        + [
            pltpu.VMEM(x.shape, x.dtype),
            pltpu.VMEM((rows, cols), F32),
            pltpu.VMEM((2, steps * cols, rows // CHUNKS), F32),
            pltpu.VMEM((owners, steps * slots, cols), F32),
            pltpu.VMEM(g.shape, g.dtype),
            pltpu.VMEM(dct.shape, dct.dtype),
            pltpu.VMEM(select.shape[1:], jnp.int32),
            pltpu.VMEM(select.shape[1:], jnp.int32),
            pltpu.SMEM(select.shape[1:], jnp.int32),
            pltpu.SemaphoreType.DMA((CHUNKS, 2)),
            pltpu.SemaphoreType.DMA((3,)),
        ],
        compiler_params=PARAMS,
        name="forward",
    )(hbm(select), hbm(x), hbm(g), hbm(m), hbm(dct))


def inverse_tile(value, row_table, col_table):
    return left(row_table, right(value, col_table))


def inverse_kernel(dct, *refs):
    coeffs, (out, held, sems) = refs[:-3], refs[-3:]
    row_table, table = left_table(dct[2], dct[3]), right_table(dct[0], dct[1])
    rows, cols = out.shape
    width = rows // len(coeffs)
    part = rows // sems.shape[0]
    copies = []
    for r in range(0, rows, cols):
        source = coeffs[r // width]
        held[r : r + cols] = inverse_tile(
            source[r % width : r % width + cols], row_table, table
        )
        if (r + cols) % part == 0:
            span = pl.ds(r + cols - part, part)
            copy = pltpu.make_async_copy(held.at[span], out.at[span], sems.at[r // part])
            copy.start()
            copies.append(copy)
    for copy in copies:
        copy.wait()


def inverse(coeffs, dct, rows):
    cols = coeffs[0].shape[1]
    return pl.pallas_call(
        inverse_kernel,
        out_shape=jax.ShapeDtypeStruct((rows, cols), F32),
        in_specs=[IN_VMEM] * (1 + len(coeffs)),
        out_specs=IN_HBM,
        scratch_shapes=[pltpu.VMEM((rows, cols), F32), pltpu.SemaphoreType.DMA((4,))],
        compiler_params=PARAMS,
        name="inverse",
    )(dct, *[vmem(c) for c in coeffs])


def class_kernel(inner, listed, dct, *refs):
    blocks, out, ordered = refs[-3::-1], refs[-2], refs[-1]
    me = lax.axis_index("dp")
    rows, cols = out.shape
    per_class, slots = listed.shape
    per_owner = rows // per_class
    replicas = len(blocks) * inner
    each = slots // replicas
    for k, block in enumerate(blocks):
        for j in range(inner):
            replica = (me // inner ^ k) * inner + (me % inner ^ j)
            span = pl.ds(pl.multiple_of(replica * each, each), each)
            for o in range(per_class):
                ordered[o, span, :] = split(block[pl.ds((j * per_class + o) * each, each), :], 1)
    ids = lax.broadcasted_iota(jnp.int32, (per_owner, slots), 0)
    sums = []
    for o in range(per_class):
        onehot = jnp.where(ids == listed[pl.ds(o, 1), :], 1.0, 0.0).astype(BF16)
        sums.append(add_columns(mm(onehot, ordered[o])))
    total = jnp.concatenate(sums, axis=0)
    row_table, table = left_table(dct[2], dct[3]), right_table(dct[0], dct[1])
    for r in range(0, rows, cols):
        out[r : r + cols] = inverse_tile(total[r : r + cols], row_table, table)


def class_rows(listed, blocks, dct, inner, rows):
    cols = blocks[0].shape[1]
    per_class, slots = listed.shape
    return pl.pallas_call(
        functools.partial(class_kernel, inner),
        out_shape=pltpu.VMEM((rows, cols), F32),
        in_specs=[IN_VMEM] * (2 + len(blocks)),
        out_specs=IN_VMEM,
        scratch_shapes=[
            pltpu.VMEM((per_class, slots, 2 * cols), BF16),
        ],
        compiler_params=PARAMS,
        name="class_rows",
    )(listed, dct, *[vmem(b) for b in reversed(blocks)])


def finish_kernel(half, count, *refs):
    blocks, (out, held, sems) = refs[count - 1 :: -1], refs[-3:]
    me = lax.axis_index("dp")
    copies = []
    for j, block in enumerate(blocks):
        held[j] = block[...].astype(held.dtype)
        copy = pltpu.make_async_copy(held.at[j], out.at[me % count ^ j, half], sems.at[j])
        copy.start()
        copies.append(copy)
    for copy in copies:
        copy.wait()


def finish(half, blocks, earlier=None):
    kept = [] if earlier is None else [earlier]
    count, shape = len(blocks), blocks[0].shape
    return pl.pallas_call(
        functools.partial(finish_kernel, half, count),
        out_shape=jax.ShapeDtypeStruct((count, HALVES) + shape, BF16),
        in_specs=[IN_VMEM] * count + [IN_HBM] * len(kept),
        out_specs=IN_HBM,
        input_output_aliases={count: 0} if kept else {},
        scratch_shapes=[pltpu.VMEM((count,) + shape, BF16), pltpu.SemaphoreType.DMA((count,))],
        compiler_params=PARAMS,
        name="finish",
    )(*[vmem(b) for b in reversed(blocks)], *kept)


def inner_size(owners):
    inner = 1
    while inner * inner < owners:
        inner *= 2
    return inner


def per_device(inputs, grad_out, momentum, select):
    replica = lax.axis_index("dp")
    owners = lax.axis_size("dp")
    rows, cols = momentum.shape[1:]
    inner = inner_size(owners)
    outer = owners // inner
    dct = tables(cols)

    def from_peer(value, shift):
        return lax.ppermute(value, "dp", [(d, d ^ shift) for d in range(owners)])

    def from_peers(values, stride):
        got = [values[0]]
        for j in range(1, len(values)):
            got.append(from_peer(values[j], j * stride))
        return got

    made = forward(
        jnp.swapaxes(select, 2, 3), inputs[0], grad_out[0], momentum[0], dct, inner
    )
    picks, rest = made[:inner], made[inner:]
    listed = jnp.transpose(select, (2, 0, 1, 3)).reshape(owners, -1)
    listed = lax.dynamic_slice_in_dim(listed, replica % inner * outer, outer, 0)
    peers = from_peers(picks, 1)
    each = owners // inner // HALVES
    lines, outs, planes = [], [], []
    for h in range(HALVES):
        span = slice(h * picks[0].shape[0] // HALVES, (h + 1) * picks[0].shape[0] // HALVES)
        planes.append(jnp.concatenate([p[span] for p in peers]))
    slots_of = [listed[h * each : (h + 1) * each] for h in range(HALVES)]
    planes[0], *slots_of = lax.optimization_barrier((planes[0], *slots_of))
    for h in range(HALVES):
        lines.append(from_peers([planes[h]] * outer, inner))
    for h in range(HALVES):
        own = class_rows(
            slots_of[h], lines[h], dct, inner, rows // inner // HALVES
        )
        outs.append(from_peers([own] * inner, 1))
    new_momentum = inverse(rest, dct, rows)
    update = None
    for h, blocks in enumerate(outs):
        update = finish(h, blocks, update)
    return (update.reshape(rows, cols), new_momentum[None])


def solution(mesh):
    return jax.shard_map(
        per_device,
        mesh=mesh,
        in_specs=(
            P("dp", None, None, None),
            P("dp", None, None, "mp"),
            P("dp", None, "mp"),
            P(None, None, None, "mp"),
        ),
        out_specs=(P(None, "mp"), P("dp", None, "mp")),
        check_vma=False,
    )
```
